16 devices in a mesh: data: 16 (over z, y, x, core).
Axes of the slice: x: 2, y: 2, z: 2, core: 2. Of those that a mesh axis runs over, the one named last changes fastest.
Arguments:
- h_a: bfloat16 [8192, 512], P('data')
- h_b: bfloat16 [8192, 512], P('data')
- w_one: bfloat16 [512, 4096], replicated
- w_two: bfloat16 [4096, 4096], replicated
- w_three: bfloat16 [4096, 4096], replicated
- gain_one: float32 [4096], replicated
- shift_one: float32 [4096], replicated
- gain_two: float32 [4096], replicated
- shift_two: float32 [4096], replicated
- lam_off: float32 [], replicated
Outputs:
- output 1: float32 [], replicated
- output 2: float32 [512, 4096], P('data')
- output 3: float32 [4096, 4096], P('data')
- output 4: float32 [4096, 4096], P('data')
- output 5: float32 [4096], replicated
- output 6: float32 [4096], replicated
- output 7: float32 [4096], replicated
- output 8: float32 [4096], replicated
All inputs are finite; a program needn't handle non-finite values.
Results may differ from the reference program's by a relative error of at most 0.00508377.
Values are sent between devices in bfloat16 or wider.
A program may use at most 1 GiB of HBM per device.

```python
import jax
import jax.numpy as jnp
from jax import lax

FEAT_DIM = 512
PROJ_DIM = 4096
ROWS_DEV = 512
SHARDS = 16
TOTAL_ROWS = ROWS_DEV * SHARDS
NORM_EPS = 1e-5


def setup_inputs(seed: int = 0) -> dict:
    key_list = jax.random.split(jax.random.key(seed), 14)
    common = jax.random.normal(key_list[0], (TOTAL_ROWS, FEAT_DIM), jnp.float32)
    shard_shift = 0.6 * jax.random.normal(key_list[1], (SHARDS, 1, FEAT_DIM), jnp.float32)
    shard_scale = jnp.exp(0.3 * jax.random.normal(key_list[2], (SHARDS, 1, FEAT_DIM), jnp.float32))

    def make_view(view_key):
        noise_vals = jax.random.normal(view_key, (TOTAL_ROWS, FEAT_DIM), jnp.float32)
        mixed_rows = (0.77 * common + 0.64 * noise_vals).reshape(SHARDS, ROWS_DEV, FEAT_DIM)
        return (mixed_rows * shard_scale + shard_shift).reshape(TOTAL_ROWS, FEAT_DIM).astype(jnp.bfloat16)

    def make_weight(weight_key, fan_in, fan_out):
        weight_scale = fan_in ** -0.5
        return (jax.random.normal(weight_key, (fan_in, fan_out), jnp.float32) * weight_scale).astype(jnp.bfloat16)

    def make_vector(vec_key, center):
        return center + 0.25 * jax.random.normal(vec_key, (PROJ_DIM,), jnp.float32)

    lam_off = (0.1 + 0.2 * jax.random.uniform(key_list[12], (), jnp.float32)) * TOTAL_ROWS / PROJ_DIM
    return {
        "h_a": make_view(key_list[3]),
        "h_b": make_view(key_list[4]),
        "w_one": make_weight(key_list[5], FEAT_DIM, PROJ_DIM),
        "w_two": make_weight(key_list[6], PROJ_DIM, PROJ_DIM),
        "w_three": make_weight(key_list[7], PROJ_DIM, PROJ_DIM),
        "gain_one": make_vector(key_list[8], 1.0),
        "shift_one": make_vector(key_list[9], 0.0),
        "gain_two": make_vector(key_list[10], 1.0),
        "shift_two": make_vector(key_list[11], 0.0),
        "lam_off": lam_off,
    }


def batch_norm(values):
    col_mean = jnp.sum(values, axis=0) / TOTAL_ROWS
    col_var = jnp.sum(values * values, axis=0) / TOTAL_ROWS - col_mean * col_mean
    return (values - col_mean) * lax.rsqrt(col_var + NORM_EPS)


def project(feat_rows, params):
    w_one, w_two, w_three, gain_one, shift_one, gain_two, shift_two = params
    hidden_one = jnp.dot(feat_rows.astype(jnp.float32), w_one, preferred_element_type=jnp.float32)
    act_one = jax.nn.relu(gain_one * batch_norm(hidden_one) + shift_one).astype(jnp.bfloat16)
    hidden_two = jnp.dot(act_one.astype(jnp.float32), w_two, preferred_element_type=jnp.float32)
    act_two = jax.nn.relu(gain_two * batch_norm(hidden_two) + shift_two).astype(jnp.bfloat16)
    proj_out = jnp.dot(act_two.astype(jnp.float32), w_three, preferred_element_type=jnp.float32)
    return batch_norm(proj_out).astype(jnp.bfloat16)


def barlow_loss(params, h_a, h_b, lam_off):
    embed_a = project(h_a, params).astype(jnp.float32)
    embed_b = project(h_b, params).astype(jnp.float32)
    corr_mat = jnp.dot(embed_a.T, embed_b, preferred_element_type=jnp.float32) / TOTAL_ROWS
    feat_index = jnp.arange(PROJ_DIM)
    diag_mask = feat_index[:, None] == feat_index[None, :]
    diag_gap = 1.0 - jnp.diagonal(corr_mat)
    off_square = jnp.sum(jnp.where(diag_mask, 0.0, corr_mat * corr_mat))
    return jnp.sum(diag_gap * diag_gap) + lam_off * off_square


def reference(h_a, h_b, w_one, w_two, w_three, gain_one, shift_one, gain_two, shift_two, lam_off):
    params = (w_one.astype(jnp.float32), w_two.astype(jnp.float32), w_three.astype(jnp.float32),
              gain_one, shift_one, gain_two, shift_two)
    loss_total, grad_list = jax.value_and_grad(barlow_loss)(params, h_a, h_b, lam_off)
    return (loss_total, grad_list[0], grad_list[1], grad_list[2],
            grad_list[3], grad_list[4], grad_list[5], grad_list[6])
```

```python
import functools

import jax
import jax.numpy as jnp
from jax import lax
from jax.experimental import pallas as pl
from jax.experimental.pallas import tpu as pltpu
from jax.sharding import PartitionSpec as P


NORM_EPS = 1e-5
FIRST_DIMS = (((0,), (0,)), ((), ()))
LAST_DIMS = (((1,), (1,)), ((), ()))
MESH_ID = pl.DeviceIdType.MESH

COLOURS = (((0, 1408), (1, 2, 3)), ((1408, 2816), (2, 3, 1)), ((2816, 4096), (3, 1, 2)))


def sum_kernel(shards, x_ref, o_ref, parts, total, send_one, recv_one, send_two, recv_two):
    me = lax.axis_index("data")
    width = x_ref.shape[1] // shards
    barrier = pltpu.get_barrier_semaphore()
    for step in range(1, shards):
        pl.semaphore_signal(barrier, inc=1, device_id=(me ^ step,), device_id_type=MESH_ID)
    pl.semaphore_wait(barrier, shards - 1)

    def cols(index):
        return pl.ds(pl.multiple_of(index * width, width), width)

    first = []
    for step in range(1, shards):
        peer = me ^ step
        copy = pltpu.make_async_remote_copy(
            src_ref=x_ref.at[:, cols(peer)], dst_ref=parts.at[step],
            send_sem=send_one.at[step], recv_sem=recv_one.at[step],
            device_id=(peer,), device_id_type=MESH_ID)
        copy.start()
        first.append(copy)
    for copy in first:
        copy.wait_recv()
    acc = x_ref[:, cols(me)]
    for step in range(1, shards):
        acc = acc + parts[step]
    total[...] = acc
    o_ref[:, cols(me)] = acc
    second = []
    for step in range(1, shards):
        copy = pltpu.make_async_remote_copy(
            src_ref=total, dst_ref=o_ref.at[:, cols(me)],
            send_sem=send_two.at[step], recv_sem=recv_two.at[step],
            device_id=(me ^ step,), device_id_type=MESH_ID)
        copy.start()
        second.append(copy)
    for copy in first:
        copy.wait_send()
    for copy in second:
        copy.wait()


def fast_sum(values, shards):
    rows, width = values.shape
    return pl.pallas_call(
        functools.partial(sum_kernel, shards),
        out_shape=jax.ShapeDtypeStruct(values.shape, jnp.float32),
        in_specs=[pl.BlockSpec(memory_space=pltpu.VMEM)],
        out_specs=pl.BlockSpec(memory_space=pltpu.VMEM),
        scratch_shapes=[pltpu.VMEM((shards, rows, width // shards), jnp.float32),
                        pltpu.VMEM((rows, width // shards), jnp.float32)]
        + [pltpu.SemaphoreType.DMA((shards,))] * 4,
        compiler_params=pltpu.CompilerParams(collective_id=rows, has_side_effects=True),
        cost_estimate=pl.CostEstimate(flops=2_000_000, bytes_accessed=200_000, transcendentals=0),
        name="fast_sum",
    )(values)


def product_kernel(ids_ref, left_one, left_two, right_one, right_two, o_ref):
    o_ref[0] = (lax.dot_general(left_one[...], right_one[...], FIRST_DIMS, preferred_element_type=jnp.float32)
                + lax.dot_general(left_two[...], right_two[...], FIRST_DIMS, preferred_element_type=jnp.float32))


def block_product(ids, lefts, rights, lo, hi, block):
    rows = lefts[0].shape[0]
    left_spec = pl.BlockSpec((rows, block), lambda i, ids_ref: (0, ids_ref[i]))
    right_spec = pl.BlockSpec((pl.Element(rows), pl.Element(hi - lo)), lambda i, ids_ref: (0, lo))
    count = ids.shape[0]
    return pl.pallas_call(
        product_kernel,
        grid_spec=pltpu.PrefetchScalarGridSpec(
            num_scalar_prefetch=1, grid=(count,),
            in_specs=[left_spec, left_spec, right_spec, right_spec],
            out_specs=pl.BlockSpec((1, block, hi - lo), lambda i, ids_ref: (i, 0, 0))),
        out_shape=jax.ShapeDtypeStruct((count, block, hi - lo), jnp.float32),
        cost_estimate=pl.CostEstimate(
            flops=4 * count * block * rows * (hi - lo), transcendentals=0,
            bytes_accessed=4 * rows * (count * block + hi - lo) + 4 * count * block * (hi - lo)),
        name="block_product",
    )(ids, *lefts, *rights)


def norm_forward(values, total_rows, shards):
    col_sums = jnp.concatenate([jnp.sum(values, axis=1), jnp.sum(values * values, axis=1)])
    col_sums = fast_sum(col_sums, shards)
    col_mean = col_sums[:2] / total_rows
    inv_std = lax.rsqrt(col_sums[2:] / total_rows - col_mean * col_mean + NORM_EPS)
    return (values - col_mean[:, None, :]) * inv_std[:, None, :], inv_std


def solution(mesh):
    shards = mesh.shape["data"]

    def local_step(h_a, h_b, w_one, w_two, w_three, gain_one, shift_one, gain_two, shift_two, lam_off):
        rows_dev = h_a.shape[0]
        total_rows = rows_dev * shards
        me = lax.axis_index("data")

        def bit(b):
            return (me >> b) & 1

        def swap(values, b):
            return lax.ppermute(values, "data", [(i, i ^ (1 << b)) for i in range(shards)])

        def pick(values, index, axis):
            return lax.dynamic_index_in_dim(values, index, axis=axis, keepdims=False)

        def blocks_of(order, value):
            high, low = sorted(order[1:], reverse=True)
            base = bit(0) | (value << order[0])
            return jnp.stack([base | (i << high) | (j << low) for i in (0, 1) for j in (0, 1)]).astype(jnp.int32)

        def products(flip, lefts, rights):
            outs = []
            for (lo, hi), order in COLOURS:
                ids = blocks_of(order, bit(order[0]) ^ flip)
                outs.append(block_product(ids, lefts, rights, lo, hi, lefts[0].shape[1] // shards))
            return outs

        def first_hop(sends):
            outs = []
            for send, (_, order) in zip(sends, COLOURS):
                outs.append(swap(send, order[0]))
            return outs

        def second_hop(keeps, aways):
            out = []
            for keep, away, (_, order) in zip(keeps, aways, COLOURS):
                axis = sorted(order[1:], reverse=True).index(order[1])
                shape = (2, 2) + keep.shape[1:]
                keep, away = keep.reshape(shape), away.reshape(shape)
                near = pick(keep, 1 - bit(order[1]), axis) + pick(away, 1 - bit(order[1]), axis)
                near = swap(near, order[1])
                half = pick(keep, bit(order[1]), axis) + pick(away, bit(order[1]), axis)
                out.append((half, near))
            return out

        def third_hop(pairs):
            out = []
            for (half, near), (_, order) in zip(pairs, COLOURS):
                far = pick(half, 1 - bit(order[2]), 0) + pick(near, 1 - bit(order[2]), 0)
                far = swap(far, order[2])
                out.append((pick(half, bit(order[2]), 0) + pick(near, bit(order[2]), 0), far))
            return out

        def finish(pairs):
            return jnp.concatenate([near + far for near, far in pairs], axis=1)

        def tie(*values):
            return lax.optimization_barrier(values)

        feat_rows = jnp.concatenate([h_a, h_b], axis=0)
        hidden_one = jnp.dot(feat_rows, w_one, preferred_element_type=jnp.float32).reshape(2, rows_dev, -1)
        normed_one, inv_one = norm_forward(hidden_one, total_rows, shards)
        pre_one = gain_one * normed_one + shift_one
        act_one = jax.nn.relu(pre_one).astype(jnp.bfloat16)
        hidden_two = jnp.dot(act_one, w_two, preferred_element_type=jnp.float32)
        normed_two, inv_two = norm_forward(hidden_two, total_rows, shards)
        pre_two = gain_two * normed_two + shift_two
        act_two = jax.nn.relu(pre_two).astype(jnp.bfloat16)
        proj_out = jnp.dot(act_two, w_three, preferred_element_type=jnp.float32)
        normed_out, inv_out = norm_forward(proj_out, total_rows, shards)
        embed_pair = normed_out.astype(jnp.bfloat16)

        one_all = act_one.reshape(2 * rows_dev, -1)
        two_all = act_two.reshape(2 * rows_dev, -1)
        embed_a, embed_b = embed_pair[0], embed_pair[1]
        lefts, rights = (embed_a, swap(embed_a, 0)), (embed_b, swap(embed_b, 0))
        aways = first_hop(products(1, lefts, rights))
        keeps = products(0, lefts, rights)
        corr_block = finish(third_hop(second_hop(keeps, aways))) / total_rows
        block_rows = corr_block.shape[0]
        row_index = me * block_rows + lax.broadcasted_iota(jnp.int32, corr_block.shape, 0)
        diag_mask = row_index == lax.broadcasted_iota(jnp.int32, corr_block.shape, 1)
        diag_gap = 1.0 - corr_block
        loss_cols = jnp.sum(jnp.where(diag_mask, diag_gap * diag_gap, lam_off * corr_block * corr_block), axis=0)
        grad_corr = jnp.where(diag_mask, -2.0 * diag_gap, 2.0 * lam_off * corr_block)
        grad_block = (grad_corr / total_rows).astype(jnp.bfloat16)
        grad_scaled = lax.all_gather(grad_block, "data", axis=0, tiled=True)

        grad_embed_a = lax.dot_general(embed_pair[1], grad_scaled, (((1,), (1,)), ((), ())),
                                       preferred_element_type=jnp.float32)
        grad_embed_b = jnp.dot(embed_pair[0], grad_scaled, preferred_element_type=jnp.float32)
        grad_embed = jnp.stack([grad_embed_a, grad_embed_b])
        sums_out = fast_sum(jnp.concatenate([
            jnp.sum(grad_embed, axis=1), jnp.sum(grad_embed * normed_out, axis=1),
            loss_cols[None], jnp.zeros((3, loss_cols.shape[0]), jnp.float32)]), shards)
        loss_total = jnp.sum(sums_out[4])

        def through_norm(grad_out, normed, inv_std, col_sums):
            return inv_std[:, None, :] * (
                grad_out - (col_sums[:2][:, None, :] + normed * col_sums[2:4][:, None, :]) / total_rows)

        def local_sums(grad_out, normed):
            return jnp.concatenate([jnp.sum(grad_out, axis=1), jnp.sum(grad_out * normed, axis=1)])

        grad_proj = through_norm(grad_embed, normed_out, inv_out, sums_out).astype(jnp.bfloat16)
        lefts = (two_all, swap(two_all, 0))
        proj_all = grad_proj.reshape(2 * rows_dev, -1)
        rights = (proj_all, swap(proj_all, 0))
        proj_a, proj_b = grad_proj[0], grad_proj[1]
        wide_a = lax.dot_general(proj_a, w_three, LAST_DIMS, preferred_element_type=jnp.float32)
        sends = products(1, lefts, rights)
        three_aways = first_hop(sends)
        wide_b = lax.dot_general(proj_b, w_three, LAST_DIMS, preferred_element_type=jnp.float32)
        grad_pre_two = jnp.where(pre_two > 0, jnp.stack([wide_a, wide_b]), 0.0)
        part_two, *rights = tie(local_sums(grad_pre_two, normed_two), *rights)
        sums_two = lax.psum(part_two, "data")
        three_keeps = products(0, lefts, rights)
        sums_two, *three_keeps = tie(sums_two, *three_keeps)
        grad_hidden_two = (gain_two * through_norm(grad_pre_two, normed_two, inv_two, sums_two)).astype(jnp.bfloat16)
        grad_hidden_two, *three_keeps = tie(grad_hidden_two, *three_keeps)

        lefts = (one_all, swap(one_all, 0))
        hidden_all = grad_hidden_two.reshape(2 * rows_dev, -1)
        rights = (hidden_all, swap(hidden_all, 0))
        hidden_a, hidden_b = grad_hidden_two[0], grad_hidden_two[1]
        wide_a = lax.dot_general(hidden_a, w_two, LAST_DIMS, preferred_element_type=jnp.float32)
        three_pairs = second_hop(three_keeps, three_aways)
        sends = products(1, lefts, rights)
        two_aways = first_hop(sends)
        wide_b = lax.dot_general(hidden_b, w_two, LAST_DIMS, preferred_element_type=jnp.float32)
        grad_pre_one = jnp.where(pre_one > 0, jnp.stack([wide_a, wide_b]), 0.0)
        part_one, *rights = tie(local_sums(grad_pre_one, normed_one), *rights)
        sums_one = lax.psum(part_one, "data")
        two_keeps = products(0, lefts, rights)
        sums_one, *two_keeps = tie(sums_one, *two_keeps)
        grad_hidden_one = (gain_one * through_norm(grad_pre_one, normed_one, inv_one, sums_one)).astype(jnp.bfloat16)
        one_part = lax.dot_general(feat_rows, grad_hidden_one.reshape(2 * rows_dev, -1), FIRST_DIMS,
                                   preferred_element_type=jnp.float32)
        one_part = one_part.reshape(2, 2, 2, 2, -1, one_part.shape[1])
        one_away = swap(pick(one_part, 1 - bit(0), 3), 0)
        one_half = pick(one_part, bit(0), 3) + one_away
        sends, keeps = [], []
        for (lo, hi), order in COLOURS:
            sends.append(pick(one_half, 1 - bit(order[0]), 3 - order[0])[..., lo:hi].reshape(4, -1, hi - lo))
            keeps.append(pick(one_half, bit(order[0]), 3 - order[0])[..., lo:hi].reshape(4, -1, hi - lo))
        grad_w_three = finish(third_hop(three_pairs))
        grad_w_two = finish(third_hop(second_hop(two_keeps, two_aways)))
        grad_w_one = finish(third_hop(second_hop(keeps, first_hop(sends))))

        return (loss_total, grad_w_one, grad_w_two, grad_w_three,
                sums_one[2] + sums_one[3], sums_one[0] + sums_one[1],
                sums_two[2] + sums_two[3], sums_two[0] + sums_two[1])

    row_spec = P("data", None)
    whole_mat = P(None, None)
    whole_vec = P(None)
    return jax.shard_map(
        local_step, mesh=mesh,
        in_specs=(row_spec, row_spec, whole_mat, whole_mat, whole_mat,
                  whole_vec, whole_vec, whole_vec, whole_vec, P()),
        out_specs=(P(), row_spec, row_spec, row_spec, whole_vec, whole_vec, whole_vec, whole_vec),
        check_vma=False)
```

```python
import functools

import jax
import jax.numpy as jnp
from jax import lax
from jax.experimental import pallas as pl
from jax.experimental.pallas import tpu as pltpu
from jax.sharding import PartitionSpec as P


NORM_EPS = 1e-5
FIRST_DIMS = (((0,), (0,)), ((), ()))
LAST_DIMS = (((1,), (1,)), ((), ()))
MESH_ID = pl.DeviceIdType.MESH

COLOURS = (((0, 1408), (1, 2, 3)), ((1408, 2816), (2, 3, 1)), ((2816, 4096), (3, 1, 2)))

EARLY_ROWS = 256


def sum_kernel(shards, x_ref, o_ref, parts, total, send_one, recv_one, send_two, recv_two):
    me = lax.axis_index("data")
    width = x_ref.shape[1] // shards
    barrier = pltpu.get_barrier_semaphore()
    for step in range(1, shards):
        pl.semaphore_signal(barrier, inc=1, device_id=(me ^ step,), device_id_type=MESH_ID)
    pl.semaphore_wait(barrier, shards - 1)

    def cols(index):
        return pl.ds(pl.multiple_of(index * width, width), width)

    first = []
    for step in range(1, shards):
        peer = me ^ step
        copy = pltpu.make_async_remote_copy(
            src_ref=x_ref.at[:, cols(peer)], dst_ref=parts.at[step],
            send_sem=send_one.at[step], recv_sem=recv_one.at[step],
            device_id=(peer,), device_id_type=MESH_ID)
        copy.start()
        first.append(copy)
    for copy in first:
        copy.wait_recv()
    acc = x_ref[:, cols(me)]
    for step in range(1, shards):
        acc = acc + parts[step]
    total[...] = acc
    o_ref[:, cols(me)] = acc
    second = []
    for step in range(1, shards):
        copy = pltpu.make_async_remote_copy(
            src_ref=total, dst_ref=o_ref.at[:, cols(me)],
            send_sem=send_two.at[step], recv_sem=recv_two.at[step],
            device_id=(me ^ step,), device_id_type=MESH_ID)
        copy.start()
        second.append(copy)
    for copy in first:
        copy.wait_send()
    for copy in second:
        copy.wait()


def fast_sum(values, shards):
    rows, width = values.shape
    return pl.pallas_call(
        functools.partial(sum_kernel, shards),
        out_shape=jax.ShapeDtypeStruct(values.shape, jnp.float32),
        in_specs=[pl.BlockSpec(memory_space=pltpu.VMEM)],
        out_specs=pl.BlockSpec(memory_space=pltpu.VMEM),
        scratch_shapes=[pltpu.VMEM((shards, rows, width // shards), jnp.float32),
                        pltpu.VMEM((rows, width // shards), jnp.float32)]
        + [pltpu.SemaphoreType.DMA((shards,))] * 4,
        compiler_params=pltpu.CompilerParams(collective_id=rows, has_side_effects=True),
        cost_estimate=pl.CostEstimate(flops=2_000_000, bytes_accessed=200_000, transcendentals=0),
        name="fast_sum",
    )(values)


def pick_kernel(block, ids_ref, *refs):
    sources, outs = refs[:-3], refs[-3:]
    for colour, o_ref in enumerate(outs):
        for index, ref in enumerate(sources):
            for i in range(4):
                start = pl.multiple_of(ids_ref[4 * colour + i] * block, block)
                o_ref[index, :, i * block:(i + 1) * block] = ref[:, pl.ds(start, block)]


def pick_blocks(ids, sources, tile):
    rows, width = sources[0].shape
    block = width // 16
    count = len(sources)
    return pl.pallas_call(
        functools.partial(pick_kernel, block),
        grid_spec=pltpu.PrefetchScalarGridSpec(
            num_scalar_prefetch=1, grid=(rows // tile,),
            in_specs=[pl.BlockSpec((tile, width), lambda i, ids_ref: (i, 0))] * count,
            out_specs=[pl.BlockSpec((count, tile, 4 * block), lambda i, ids_ref: (0, i, 0))] * 3),
        out_shape=[jax.ShapeDtypeStruct((count, rows, 4 * block), sources[0].dtype)] * 3,
        cost_estimate=pl.CostEstimate(flops=8_000_000, transcendentals=0,
                                      bytes_accessed=4 * count * rows * width),
        name="pick_blocks",
    )(ids, *sources)


def product_kernel(fars, ids_ref, own, core, *refs):
    far_refs = refs[:fars]
    right_own, right_core, right_far, right_cross, send_ref, keep_ref = refs[fars:]

    def dot(left, right):
        return lax.dot_general(left, right, FIRST_DIMS, preferred_element_type=jnp.float32)

    total = dot(own[...], right_own[...]) + dot(core[...], right_core[...])
    first = 0
    for far in far_refs:
        rows = far.shape[1]
        total = total + dot(far[0], right_far[first:first + rows, :]) + dot(far[1], right_cross[first:first + rows, :])
        first += rows
    step = pl.program_id(0)

    @pl.when(step < 2)
    def _():
        send_ref[0] = total

    @pl.when(step >= 2)
    def _():
        keep_ref[0] = total


def block_product(ids, colour, own, core, fars, rights):
    rows, width = rights[0].shape
    block = own.shape[1] // 16
    left_spec = pl.BlockSpec((rows, block), lambda i, ids_ref: (0, ids_ref[4 * colour + i]))
    far_specs = [pl.BlockSpec((2, far.shape[1], block), lambda i, ids_ref: (0, 0, i)) for far in fars]
    slice_spec = pl.BlockSpec((rows, width), lambda i, ids_ref: (0, 0))
    return pl.pallas_call(
        functools.partial(product_kernel, len(fars)),
        grid_spec=pltpu.PrefetchScalarGridSpec(
            num_scalar_prefetch=1, grid=(4,),
            in_specs=[left_spec, left_spec, *far_specs, *[slice_spec] * 4],
            out_specs=[pl.BlockSpec((1, block, width), lambda i, ids_ref: (jnp.minimum(i, 1), 0, 0)),
                       pl.BlockSpec((1, block, width), lambda i, ids_ref: (jnp.maximum(i - 2, 0), 0, 0))]),
        out_shape=[jax.ShapeDtypeStruct((2, block, width), jnp.float32)] * 2,
        cost_estimate=pl.CostEstimate(
            flops=32 * block * rows * width, transcendentals=0,
            bytes_accessed=8 * rows * (4 * block + width) + 16 * block * width),
        name="block_product",
    )(ids, own, core, *fars, *rights)


def layer(rows, weights):
    values = jnp.dot(rows, weights, preferred_element_type=jnp.float32)
    values = values.reshape(2, -1, values.shape[-1])
    return values, jnp.concatenate([jnp.sum(values, axis=1), jnp.sum(values * values, axis=1)])


def norm_forward(values, col_sums, total_rows, shards):
    col_sums = fast_sum(col_sums, shards)
    col_mean = col_sums[:2] / total_rows
    inv_std = lax.rsqrt(col_sums[2:] / total_rows - col_mean * col_mean + NORM_EPS)

    def normed(lo=0, hi=None, first=0):
        return (values[first:, :, lo:hi] - col_mean[first:, None, lo:hi]) * inv_std[first:, None, lo:hi]

    return normed, inv_std, col_mean


def solution(mesh):
    shards = mesh.shape["data"]

    def local_step(h_a, h_b, w_one, w_two, w_three, gain_one, shift_one, gain_two, shift_two, lam_off):
        rows_dev = h_a.shape[0]
        total_rows = rows_dev * shards
        me = lax.axis_index("data")

        def bit(b):
            return (me >> b) & 1

        def swap(values, b):
            return lax.ppermute(values, "data", [(i, i ^ (1 << b)) for i in range(shards)])

        def pick(values, index, axis):
            return lax.dynamic_index_in_dim(values, index, axis=axis, keepdims=False)

        def blocks_of(order, flip):
            base = bit(0) | ((bit(order[0]) ^ flip) << order[0])
            return jnp.stack([base | ((bit(order[1]) ^ i) << order[1]) | ((bit(order[2]) ^ j) << order[2])
                              for i in (1, 0) for j in (1, 0)]).astype(jnp.int32)

        mine = jnp.concatenate([blocks_of(order, 0) for _, order in COLOURS])
        theirs = jnp.concatenate([blocks_of(order, 1) for _, order in COLOURS])

        def exchange(values):
            outs = []
            for value, (_, order) in zip(values, COLOURS):
                outs.append(swap(value, order[0]))
            return outs

        def picks(sources):
            return pick_blocks(theirs, sources, 128)

        def products(own, core, fars, slices, right_cores, right_fars, crosses):
            outs = []
            for index in range(3):
                rights = (slices[index], right_cores[index], right_fars[index], crosses[index])
                outs.append(block_product(mine, index, own, core, fars[index], rights))
            return outs

        def second_hop(pairs):
            outs = []
            for (send, keep), (_, order) in zip(pairs, COLOURS):
                outs.append((keep, swap(send, order[1])))
            return outs

        def third_hop(pairs):
            outs = []
            for (half, near), (_, order) in zip(pairs, COLOURS):
                send, held = half[0] + near[0], half[1] + near[1]
                far = swap(send, order[2])
                outs.append((held, far))
            return outs

        def finish(pairs):
            return jnp.concatenate([near + far for near, far in pairs], axis=1)

        def tie(*values):
            return lax.optimization_barrier(values)

        feat_rows = jnp.concatenate([h_a, h_b], axis=0)
        normed_one, inv_one, mean_one = norm_forward(*layer(feat_rows, w_one), total_rows, shards)

        def pre_one(lo=0, hi=None):
            return gain_one[lo:hi] * normed_one(lo, hi) + shift_one[lo:hi]

        act_one = jax.nn.relu(pre_one()).astype(jnp.bfloat16)
        feat_late, _ = tie(feat_rows, inv_one)
        feat_fars = exchange([feat_late] * 3)
        normed_two, inv_two, _ = norm_forward(*layer(act_one, w_two), total_rows, shards)

        def pre_two(lo=0, hi=None):
            return gain_two[lo:hi] * normed_two(lo, hi) + shift_two[lo:hi]

        act_two = jax.nn.relu(pre_two()).astype(jnp.bfloat16)
        two_all = act_two.reshape(2 * rows_dev, -1)
        early = two_all[:EARLY_ROWS]
        two_early = exchange(picks((early, swap(early, 0))))
        normed_out, inv_out, _ = norm_forward(*layer(act_two, w_three), total_rows, shards)
        slices = [tie(normed_out(lo, hi, 1)[0].astype(jnp.bfloat16))[0] for (lo, hi), _ in COLOURS]
        embed_pair = normed_out().astype(jnp.bfloat16)

        one_all = act_one.reshape(2 * rows_dev, -1)
        embed_a = embed_pair[0]
        right_fars = exchange(slices)
        crosses = [swap(value, 0) for value in right_fars]
        core_a = swap(embed_a, 0)
        fars = exchange(picks((embed_a, core_a)))

        vectors = jnp.concatenate([mean_one, inv_one, gain_one[None], shift_one[None],
                                   jnp.zeros((2, gain_one.shape[0]), jnp.float32)])
        one_weights = pick_blocks(mine, (w_one,), 128)
        one_scales = pick_blocks(mine, (vectors,), 8)
        one_fars = []
        for index in range(3):
            weights, scales = one_weights[index][0], one_scales[index][0]
            rows = jnp.concatenate([feat_fars[index], swap(feat_fars[index], 0)], axis=0)
            hidden = jnp.dot(rows, weights, preferred_element_type=jnp.float32).reshape(2, 2, rows_dev, -1)
            normed = (hidden - scales[None, 0:2, None]) * scales[None, 2:4, None]
            far = jax.nn.relu(scales[4] * normed + scales[5]).astype(jnp.bfloat16)
            one_fars.append([far.reshape(2, 2 * rows_dev, -1)])

        pairs = products(embed_a, core_a, [[far] for far in fars], slices, [swap(value, 0) for value in slices], right_fars, crosses)
        corr_block = finish(third_hop(second_hop(pairs))) / total_rows
        block_rows = corr_block.shape[0]
        row_index = me * block_rows + lax.broadcasted_iota(jnp.int32, corr_block.shape, 0)
        diag_mask = row_index == lax.broadcasted_iota(jnp.int32, corr_block.shape, 1)
        diag_gap = 1.0 - corr_block
        loss_cols = jnp.sum(jnp.where(diag_mask, diag_gap * diag_gap, lam_off * corr_block * corr_block), axis=0)
        grad_corr = jnp.where(diag_mask, -2.0 * diag_gap, 2.0 * lam_off * corr_block)
        grad_block = (grad_corr / total_rows).astype(jnp.bfloat16)
        grad_scaled = lax.all_gather(grad_block, "data", axis=0, tiled=True)

        late = two_all[EARLY_ROWS:]
        late = picks((late, swap(late, 0)))
        two_core, one_core = swap(two_all, 0), swap(one_all, 0)
        ready = tie(grad_scaled, *late, *[far for pair in one_fars for far in pair], two_all, two_core, one_all, one_core)
        grad_scaled, late, one_fars = ready[0], ready[1:4], [[far] for far in ready[4:7]]
        two_all, two_core, one_all, one_core = ready[7:]
        two_late = exchange(late)
        grad_embed_a = lax.dot_general(embed_pair[1], grad_scaled, LAST_DIMS, preferred_element_type=jnp.float32)
        grad_embed_b = jnp.dot(embed_pair[0], grad_scaled, preferred_element_type=jnp.float32)
        grad_embed = jnp.stack([grad_embed_a, grad_embed_b])
        sums_out = fast_sum(jnp.concatenate([
            jnp.sum(grad_embed, axis=1), jnp.sum(grad_embed * normed_out(), axis=1),
            loss_cols[None], jnp.zeros((3, loss_cols.shape[0]), jnp.float32)]), shards)
        loss_total = jnp.sum(sums_out[4])

        def through_norm(grad_out, normed, inv_std, col_sums, lo=0, hi=None):
            return inv_std[:, None, lo:hi] * (grad_out(lo, hi) - (
                col_sums[:2, None, lo:hi] + normed(lo, hi) * col_sums[2:4, None, lo:hi]) / total_rows)

        def local_sums(grad_out, normed):
            return jnp.concatenate([jnp.sum(grad_out, axis=1), jnp.sum(grad_out * normed(), axis=1)])

        def grad_proj(lo, hi):
            return through_norm(lambda lo, hi: grad_embed[..., lo:hi], normed_out, inv_out, sums_out, lo, hi)

        def weight_products(grads, weights, own, core, fars, pre, normed):
            slices = [grads(lo, hi).astype(jnp.bfloat16).reshape(2 * rows_dev, -1) for (lo, hi), _ in COLOURS]
            slices = [tie(value)[0] for value in slices]
            right_fars = exchange(slices)
            right_cores = [swap(value, 0) for value in slices]
            right, = tie(jnp.concatenate(slices, axis=1))
            wide = lax.dot_general(right, weights, LAST_DIMS, preferred_element_type=jnp.float32)
            wide = wide.reshape(2, rows_dev, -1)
            part = local_sums(jnp.where(pre() > 0, wide, 0.0), normed)
            col_sums = lax.psum(part, "data")
            crosses = [swap(value, 0) for value in right_fars]
            pairs = products(own, core, fars, slices, right_cores, right_fars, crosses)

            def grad_pre(lo=0, hi=None):
                return jnp.where(pre(lo, hi) > 0, wide[..., lo:hi], 0.0)

            return grad_pre, col_sums, second_hop(pairs)

        grad_pre_two, sums_two, three_pairs = weight_products(
            grad_proj, w_three, two_all, two_core, [list(pair) for pair in zip(two_early, two_late)], pre_two, normed_two)
        sums_two, *keeps = tie(sums_two, *[keep for keep, _ in three_pairs])
        three_pairs = [(keep, near) for keep, (_, near) in zip(keeps, three_pairs)]

        def grad_hidden_two(lo, hi):
            return gain_two[lo:hi] * through_norm(grad_pre_two, normed_two, inv_two, sums_two, lo, hi)

        grad_pre_one, sums_one, two_pairs = weight_products(
            grad_hidden_two, w_two, one_all, one_core, one_fars, pre_one, normed_one)
        sums_one, *keeps = tie(sums_one, *[keep for keep, _ in two_pairs])
        two_pairs = [(keep, near) for keep, (_, near) in zip(keeps, two_pairs)]
        grad_hidden_one = (gain_one * through_norm(grad_pre_one, normed_one, inv_one, sums_one)).astype(jnp.bfloat16)
        one_part = lax.dot_general(feat_rows, grad_hidden_one.reshape(2 * rows_dev, -1), FIRST_DIMS,
                                   preferred_element_type=jnp.float32)
        one_part = one_part.reshape(2, 2, 2, 2, -1, one_part.shape[1])
        one_away = swap(pick(one_part, 1 - bit(0), 3), 0)
        cuts = []
        for (lo, hi), order in COLOURS:
            half = pick(one_part, bit(0), 3)[..., lo:hi] + one_away[..., lo:hi]
            cuts.append([pick(half, bit(order[0]) ^ flip, 3 - order[0]) for flip in (1, 0)])
        aways = exchange([send for send, _ in cuts])
        pairs = []
        for (_, half), away, (_, order) in zip(cuts, aways, COLOURS):
            axis = sorted(order[1:], reverse=True).index(order[1])
            nearer = []
            for flip in (1, 0):
                part = pick(half, bit(order[1]) ^ flip, axis) + pick(away, bit(order[1]) ^ flip, axis)
                nearer.append(jnp.stack([pick(part, 1 - bit(order[2]), 0), pick(part, bit(order[2]), 0)]))
            pairs.append(nearer)
        grad_w_three = finish(third_hop(three_pairs))
        grad_w_two = finish(third_hop(two_pairs))
        grad_w_one = finish(third_hop(second_hop(pairs)))

        return (loss_total, grad_w_one, grad_w_two, grad_w_three,
                sums_one[2] + sums_one[3], sums_one[0] + sums_one[1],
                sums_two[2] + sums_two[3], sums_two[0] + sums_two[1])

    row_spec = P("data", None)
    whole_mat = P(None, None)
    whole_vec = P(None)
    return jax.shard_map(
        local_step, mesh=mesh,
        in_specs=(row_spec, row_spec, whole_mat, whole_mat, whole_mat,
                  whole_vec, whole_vec, whole_vec, whole_vec, P()),
        out_specs=(P(), row_spec, row_spec, row_spec, whole_vec, whole_vec, whole_vec, whole_vec),
        check_vma=False)
```
